128 devices in a mesh: emb: 128 (over z, y, x, core).
Axes of the slice: x: 4, y: 4, z: 4, core: 2. Of those that a mesh axis runs over, the one named last changes fastest.
Arguments:
- token_ids: int32 [16384], P('emb')
- hot_ids: int32 [2048], replicated
- x_in: bfloat16 [16384, 3072], P('emb')
- d_out: bfloat16 [16384, 3072], P('emb')
- emb_table: bfloat16 [2, 128256, 256], P(None, 'emb')
- hot_table: bfloat16 [2, 2048, 256], replicated
- w_up: bfloat16 [2, 3072, 8192], replicated
- w_down: bfloat16 [2, 8192, 3072], replicated
- w_gate: bfloat16 [2, 3072, 256], replicated
- w_proj: bfloat16 [2, 256, 3072], replicated
Outputs:
- output 1: bfloat16 [16384, 3072], P('emb')
- output 2: float32 [2, 128256, 256], P(None, 'emb')
- output 3: float32 [2, 2048, 256], replicated
All inputs are finite; a program needn't handle non-finite values.
Results may differ from the reference program's by a relative error of at most 0.0121393.
Values are sent between devices in bfloat16 or wider.
A program may use at most 1 GiB of HBM per device.

```python
import math
import jax
import jax.numpy as jnp
from jax import lax

TOKENS = 128
SHARDS = 128
MODEL_DIM = 3072
FF_DIM = 8192
EMB_DIM = 256
VOCAB_SIZE = 128256
HOT_ROWS = 2048
LAYERS = 2

NORM_EPS = 1e-6
TOKENS_ALL = TOKENS * SHARDS
ROWS_DEV = VOCAB_SIZE // SHARDS
CAPACITY = max(8, (2 * TOKENS) // SHARDS)
LOG_VOCAB = int(math.log2(VOCAB_SIZE))


def draw_token_ids(key):
    k_perm, k_level, k_draw = jax.random.split(key, 3)
    perm_ids = jax.random.permutation(k_perm, VOCAB_SIZE).astype(jnp.int32)
    level = jax.random.randint(k_level, (TOKENS_ALL,), 0, LOG_VOCAB + 1)
    raw_draw = jax.random.randint(k_draw, (TOKENS_ALL,), 0, VOCAB_SIZE)
    span = jnp.minimum(jnp.left_shift(jnp.ones_like(level), level), VOCAB_SIZE)
    position = jnp.arange(TOKENS_ALL, dtype=jnp.int32)
    freq_rank = jnp.where(position % TOKENS < CAPACITY, HOT_ROWS, raw_draw % span)
    is_cold = freq_rank >= HOT_ROWS
    owner_id = perm_ids[freq_rank] // ROWS_DEV
    group_key = jnp.where(is_cold, (position // TOKENS) * SHARDS + owner_id, SHARDS * SHARDS)
    order = jnp.argsort(group_key, stable=True)
    sorted_key = group_key[order]
    group_start = jnp.searchsorted(sorted_key, sorted_key, side='left').astype(jnp.int32)
    within = jnp.zeros((TOKENS_ALL,), jnp.int32).at[order].set(position - group_start)
    freq_rank = jnp.where(is_cold & (within >= CAPACITY), position % HOT_ROWS, freq_rank)
    return perm_ids[freq_rank], perm_ids[:HOT_ROWS]


def normal_init(key, shape, scale):
    return (jax.random.normal(key, shape, jnp.float32) * scale).astype(jnp.bfloat16)


def setup_inputs(seed: int = 0) -> dict:
    keys = jax.random.split(jax.random.key(seed), 10)
    token_ids, hot_ids = draw_token_ids(keys[0])
    return {
        'token_ids': token_ids,
        'hot_ids': hot_ids,
        'x_in': normal_init(keys[1], (TOKENS_ALL, MODEL_DIM), 1.0),
        'd_out': normal_init(keys[2], (TOKENS_ALL, MODEL_DIM), 1.0),
        'emb_table': normal_init(keys[3], (LAYERS, VOCAB_SIZE, EMB_DIM), 1.0),
        'hot_table': normal_init(keys[4], (LAYERS, HOT_ROWS, EMB_DIM), 1.0),
        'w_up': normal_init(keys[5], (LAYERS, MODEL_DIM, FF_DIM), MODEL_DIM ** -0.5),
        'w_down': normal_init(keys[6], (LAYERS, FF_DIM, MODEL_DIM), 0.5 * FF_DIM ** -0.5),
        'w_gate': normal_init(keys[7], (LAYERS, MODEL_DIM, EMB_DIM), MODEL_DIM ** -0.5),
        'w_proj': normal_init(keys[8], (LAYERS, EMB_DIM, MODEL_DIM), 0.5 * EMB_DIM ** -0.5),
    }


def gelu_back(pre_act, cot_in):
    _, pull = jax.vjp(jax.nn.gelu, pre_act.astype(jnp.float32))
    return pull(cot_in)[0]


def dense_parts(resid, w_up, w_gate):
    resid_f = resid.astype(jnp.float32)
    inv_rms = lax.rsqrt(jnp.mean(resid_f * resid_f, axis=-1, keepdims=True) + NORM_EPS)
    normed = (resid_f * inv_rms).astype(jnp.bfloat16)
    hidden = jnp.dot(normed, w_up, preferred_element_type=jnp.float32).astype(jnp.bfloat16)
    gate_pre = jnp.dot(normed, w_gate, preferred_element_type=jnp.float32).astype(jnp.bfloat16)
    return resid_f, inv_rms, hidden, gate_pre


def layer_forward(resid, emb_rows, w_up, w_down, w_gate, w_proj):
    resid_f, _, hidden, gate_pre = dense_parts(resid, w_up, w_gate)
    activated = jax.nn.gelu(hidden.astype(jnp.float32)).astype(jnp.bfloat16)
    mlp_out = jnp.dot(activated, w_down, preferred_element_type=jnp.float32).astype(jnp.bfloat16)
    gate = jax.nn.gelu(gate_pre.astype(jnp.float32)).astype(jnp.bfloat16)
    mixed = (gate.astype(jnp.float32) * emb_rows.astype(jnp.float32)).astype(jnp.bfloat16)
    projected = jnp.dot(mixed, w_proj, preferred_element_type=jnp.float32).astype(jnp.bfloat16)
    return (resid_f + mlp_out.astype(jnp.float32) + projected.astype(jnp.float32)).astype(jnp.bfloat16)


def layer_backward(resid, emb_rows, d_next, w_up, w_down, w_gate, w_proj):
    resid_f, inv_rms, hidden, gate_pre = dense_parts(resid, w_up, w_gate)
    gate = jax.nn.gelu(gate_pre.astype(jnp.float32)).astype(jnp.bfloat16)
    d_cast = d_next.astype(jnp.bfloat16)
    d_mixed = jnp.dot(d_cast, w_proj.T, preferred_element_type=jnp.float32)
    d_rows = gate.astype(jnp.float32) * d_mixed
    d_gpre = gelu_back(gate_pre, d_mixed * emb_rows.astype(jnp.float32))
    d_hidden = gelu_back(hidden, jnp.dot(d_cast, w_down.T, preferred_element_type=jnp.float32))
    d_normed = (jnp.dot(d_hidden.astype(jnp.bfloat16), w_up.T, preferred_element_type=jnp.float32)
                + jnp.dot(d_gpre.astype(jnp.bfloat16), w_gate.T, preferred_element_type=jnp.float32))
    inner = jnp.mean(d_normed * resid_f, axis=-1, keepdims=True)
    d_prev = d_next + inv_rms * d_normed - resid_f * (inv_rms * inv_rms * inv_rms) * inner
    return d_prev, d_rows


def reference(token_ids, hot_ids, x_in, d_out, emb_table, hot_table, w_up, w_down, w_gate, w_proj):
    slot_map = jnp.full((VOCAB_SIZE,), -1, jnp.int32).at[hot_ids].set(jnp.arange(HOT_ROWS, dtype=jnp.int32))
    hot_slot = slot_map[token_ids]
    is_hot = hot_slot >= 0
    hot_slot = jnp.maximum(hot_slot, 0)

    def fwd_step(resid, layer_w):
        table_l, hot_l, up_l, down_l, gate_l, proj_l = layer_w
        emb_rows = jnp.where(is_hot[:, None], hot_l[hot_slot], table_l[token_ids])
        return layer_forward(resid, emb_rows, up_l, down_l, gate_l, proj_l), (resid, emb_rows)

    x_out, (x_saved, rows_saved) = lax.scan(fwd_step, x_in, (emb_table, hot_table, w_up, w_down, w_gate, w_proj))

    def bwd_step(d_resid, layer_w):
        resid_l, rows_l, up_l, down_l, gate_l, proj_l = layer_w
        d_prev, d_rows = layer_backward(resid_l, rows_l, d_resid, up_l, down_l, gate_l, proj_l)
        hot_part = jnp.where(is_hot[:, None], d_rows, 0.0)
        d_tab = jax.ops.segment_sum(d_rows - hot_part, token_ids, num_segments=VOCAB_SIZE)
        d_hot_l = jax.ops.segment_sum(hot_part, hot_slot, num_segments=HOT_ROWS)
        return d_prev, (d_tab, d_hot_l)

    _, (d_table, d_hot) = lax.scan(bwd_step, d_out.astype(jnp.float32), (x_saved, rows_saved, w_up, w_down, w_gate, w_proj), reverse=True)
    return x_out, d_table, d_hot
```

```python
import functools

import jax
import jax.numpy as jnp
from jax import lax
from jax.experimental import pallas as pl
from jax.experimental.pallas import tpu as pltpu
from jax.sharding import PartitionSpec as P

NORM_EPS = 1e-6
MESH = pl.DeviceIdType.MESH
F32, BF16, I32 = jnp.float32, jnp.bfloat16, jnp.int32
ANY = pl.BlockSpec(memory_space=pl.ANY)
VM = pl.BlockSpec(memory_space=pltpu.VMEM)
GC = 0.7978845608028654
VMEM_LIMIT = 60 * 1024 * 1024


def dot_nn(a, b):
    return jnp.dot(a, b, preferred_element_type=F32)


def dot_nt(a, b):
    return lax.dot_general(a, b, (((1,), (1,)), ((), ())), preferred_element_type=F32)


def gelu(x):
    return 0.5 * x * (1.0 + jnp.tanh(GC * (x + 0.044715 * x * x * x)))


def gelu_both(x):
    x2 = x * x
    t = jnp.tanh(GC * (x + 0.044715 * x * x2))
    half = 0.5 * (1.0 + t)
    return x * half, half + 0.5 * x * (1.0 - t * t) * (GC * (1.0 + 3.0 * 0.044715 * x2))


def rms(xf):
    return lax.rsqrt(jnp.mean(xf * xf, axis=-1, keepdims=True) + NORM_EPS)


def pieces(x):
    hi = x.astype(BF16)
    rest = x - hi.astype(F32)
    mid = rest.astype(BF16)
    return hi, mid, (rest - mid.astype(F32)).astype(BF16)


def dot3(oh, x):
    hi, mid, lo = pieces(x)
    return dot_nn(oh, hi) + dot_nn(oh, mid) + dot_nn(oh, lo)


def rcopy(src, dst, ssem, rsem, dev):
    return pltpu.make_async_remote_copy(src_ref=src, dst_ref=dst, send_sem=ssem, recv_sem=rsem,
                                        device_id=(dev,), device_id_type=MESH)


def pair_barrier(partner):
    bar = pltpu.get_barrier_semaphore()
    pl.semaphore_signal(bar, inc=1, device_id=(partner,), device_id_type=MESH)
    return bar


N_UP = 8
N_DN = 6
SLOTS = 3


def k0_body(x_ref, wg_ref, wup, wdn, m_ref, g_ref, xp, up, act, wu, wd, msend, mown, mrecv,
            su, sd, xs, xr, ms, mr):
    tok, dim = x_ref.shape
    half = act.shape[1]
    fu, nd = half // N_UP, dim // N_DN
    me = lax.axis_index('emb')
    par = lax.rem(me, 2)
    partner = me + 1 - 2 * par
    base = par * half

    def up_copy(i, slot):
        return pltpu.make_async_copy(wup.at[0, :, pl.ds(pl.multiple_of(base + i * fu, fu), fu)], wu.at[slot], su.at[slot])

    def dn_copy(i, slot):
        return pltpu.make_async_copy(wdn.at[0, pl.ds(pl.multiple_of(base, half), half), pl.ds(pl.multiple_of(i * nd, nd), nd)],
                                     wd.at[slot], sd.at[slot])

    for i in range(SLOTS):
        up_copy(i, i).start()
    bar = pair_barrier(partner)
    pl.semaphore_wait(bar, 1)
    xsend = rcopy(x_ref, xp, xs, xr, partner)
    xsend.start()
    xf = x_ref[...].astype(F32)
    u = (xf * rms(xf)).astype(BF16)
    up[pl.ds(0, tok), :] = u
    g_ref[...] = gelu(dot_nn(u, wg_ref[...]).astype(BF16).astype(F32)).astype(BF16)
    xsend.wait()
    xf = xp[...].astype(F32)
    up[pl.ds(tok, tok), :] = (xf * rms(xf)).astype(BF16)

    def up_step(i, c):
        slot = lax.rem(i, SLOTS)
        up_copy(i, slot).wait()
        h = dot_nn(up[...], wu[slot]).astype(BF16).astype(F32)
        act[:, pl.ds(pl.multiple_of(i * fu, fu), fu)] = gelu(h).astype(BF16)

        @pl.when(i + SLOTS < N_UP)
        def _():
            up_copy(i + SLOTS, slot).start()

        @pl.when(i + SLOTS >= N_UP)
        def _():
            dn_copy(i + SLOTS - N_UP, i + SLOTS - N_UP).start()
        return c

    lax.fori_loop(0, N_UP, up_step, 0)

    def dn_step(i, c):
        slot = lax.rem(i, SLOTS)
        dn_copy(i, slot).wait()
        r = dot_nn(act[...], wd[slot])
        mown[i] = r[:tok]
        msend[i] = r[tok:]
        rcopy(msend.at[i], mrecv.at[i], ms.at[i], mr.at[i], partner).start()

        @pl.when(i + SLOTS < N_DN)
        def _():
            dn_copy(i + SLOTS, slot).start()
        return c

    lax.fori_loop(0, N_DN, dn_step, 0)
    for i in range(N_DN):
        rcopy(msend.at[i], mrecv.at[i], ms.at[i], mr.at[i], partner).wait()
        m_ref[:, i * nd:(i + 1) * nd] = (mown[i] + mrecv[i]).astype(BF16)


def k1_body(x_ref, m0_ref, g0_ref, e0_ref, e1_ref, d_ref, wp0_ref, wg1_ref, wp1_ref, wup, wdn,
            xo_ref, rows0_ref, rows1_ref, x1, x1p, cp, up, macc, dacc, mrecv, drecv, wu, wd,
            su, sd, xs, xr, cs, cr, ms, mr, ds, dr):
    tok, dim = x_ref.shape
    ff = wup.shape[2]
    half = ff // 2
    fu = half // N_UP
    me = lax.axis_index('emb')
    par = lax.rem(me, 2)
    partner = me + 1 - 2 * par
    base = par * half

    def up_copy(i, slot):
        return pltpu.make_async_copy(wup.at[1, :, pl.ds(pl.multiple_of(base + i * fu, fu), fu)], wu.at[slot], su.at[slot])

    def dn_copy(i, slot):
        return pltpu.make_async_copy(wdn.at[1, pl.ds(pl.multiple_of(base + i * fu, fu), fu), :], wd.at[slot], sd.at[slot])

    for i in range(SLOTS):
        up_copy(i, i).start()
        dn_copy(i, i).start()
    bar = pair_barrier(partner)
    pl.semaphore_wait(bar, 1)
    csend = rcopy(d_ref, cp.at[pl.ds(tok, tok)], cs, cr, partner)
    csend.start()
    cp[pl.ds(0, tok), :] = d_ref[...]
    q = dot_nn((g0_ref[...].astype(F32) * e0_ref[...].astype(F32)).astype(BF16), wp0_ref[...]).astype(BF16)
    x1[...] = (x_ref[...].astype(F32) + m0_ref[...].astype(F32) + q.astype(F32)).astype(BF16)
    xsend = rcopy(x1, x1p, xs, xr, partner)
    xsend.start()
    xf = x1[...].astype(F32)
    u = (xf * rms(xf)).astype(BF16)
    up[pl.ds(0, tok), :] = u
    s1 = dot_nn(u, wg1_ref[...]).astype(BF16).astype(F32)
    gs, dgs = gelu_both(s1)
    g1 = gs.astype(BF16).astype(F32)
    a1 = dot_nt(d_ref[...], wp1_ref[...])
    rows1_ref[...] = a1 * g1
    e1 = e1_ref[...].astype(F32)
    du_gate = dot_nt((dgs * (a1 * e1)).astype(BF16), wg1_ref[...])
    dacc[pl.ds(0, tok), :] = du_gate
    dacc[pl.ds(tok, tok), :] = jnp.zeros_like(du_gate)
    macc[...] = jnp.zeros_like(macc)
    xsend.wait()
    csend.wait()
    xf = x1p[...].astype(F32)
    up[pl.ds(tok, tok), :] = (xf * rms(xf)).astype(BF16)

    def step(i, c):
        slot = lax.rem(i, SLOTS)
        up_copy(i, slot).wait()
        dn_copy(i, slot).wait()
        h = dot_nn(up[...], wu[slot]).astype(BF16).astype(F32)
        a, da = gelu_both(h)
        dh = (da * dot_nt(cp[...], wd[slot])).astype(BF16)
        macc[...] += dot_nn(a.astype(BF16), wd[slot])
        dacc[...] += dot_nt(dh, wu[slot])

        @pl.when(i + SLOTS < N_UP)
        def _():
            up_copy(i + SLOTS, slot).start()
            dn_copy(i + SLOTS, slot).start()
        return c

    lax.fori_loop(0, N_UP, step, 0)
    dsend = rcopy(dacc.at[pl.ds(tok, tok)], drecv, ds, dr, partner)
    msend = rcopy(macc.at[pl.ds(tok, tok)], mrecv, ms, mr, partner)
    dsend.start()
    msend.start()
    q1 = dot_nn((g1 * e1).astype(BF16), wp1_ref[...]).astype(BF16)
    dsend.wait()
    du = dacc[pl.ds(0, tok), :] + drecv[...]
    xf = x1[...].astype(F32)
    k = rms(xf)
    inner = jnp.mean(du * xf, axis=-1, keepdims=True)
    r1 = d_ref[...].astype(F32) + k * du - xf * (k * k * k) * inner
    rows0_ref[...] = dot_nt(r1.astype(BF16), wp0_ref[...]) * g0_ref[...].astype(F32)
    msend.wait()
    m1 = (macc[pl.ds(0, tok), :] + mrecv[...]).astype(BF16)
    xo_ref[...] = (xf + m1.astype(F32) + q1.astype(F32)).astype(BF16)


def wait_bytes(ref, sem):
    pltpu.make_async_copy(ref, ref, sem).wait()


def kh_body(rows_ref, hidx_ref, slot_ref, cold_ref, dhot_ref,
            csend, crecv, rall, iall, pown, psend, precv, tsend, trecv, dh,
            asem, ar, ai, cs, cr, ds, dr, ts, tr, gs, gr, fs, fr, osem):
    n_dev = csend.shape[0]
    tok = rows_ref.shape[0]
    me = lax.axis_index('emb')
    core = lax.rem(me, 2)
    chip = me // 2
    x = lax.rem(chip, 4)
    zy = chip // 4
    z = zy // 4
    partner = me + 1 - 2 * core
    bar = pltpu.get_barrier_semaphore()

    def sig(d, c):
        pl.semaphore_signal(bar, inc=1, device_id=(lax.rem(me + d, n_dev),), device_id_type=MESH)
        return c

    lax.fori_loop(1, n_dev, sig, 0)
    rall[x] = rows_ref[...]
    iall[x] = jnp.broadcast_to(hidx_ref[...], iall.shape[1:])
    slots = lax.broadcasted_iota(I32, (n_dev * 8, tok), 0)
    oh = jnp.where(slots == slot_ref[...], 1.0, 0.0).astype(BF16)
    csend[...] = dot3(oh, rows_ref[...]).reshape(csend.shape)
    crecv[me] = csend[me]
    pl.semaphore_wait(bar, n_dev - 1)

    def a_copies(d):
        dev = (zy * 4 + lax.rem(x + d, 4)) * 2 + core
        return (rcopy(rall.at[x], rall.at[x], asem.at[0], ar, dev),
                rcopy(iall.at[x], iall.at[x], asem.at[1], ai, dev))

    for d in (1, 3, 2):
        for cpy in a_copies(d):
            cpy.start()

    def cold(d, c):
        dev = lax.rem(me + d, n_dev)
        rcopy(csend.at[dev], crecv.at[me], cs, cr, dev).start()
        return c

    lax.fori_loop(1, n_dev // 4, cold, 0)
    wait_bytes(rall.at[pl.ds(0, 3)], ar)
    wait_bytes(iall.at[pl.ds(0, 3)], ai)
    q = lax.broadcasted_iota(I32, (256, 4 * tok), 0)
    ids = jnp.concatenate([iall[i, 0:1, :] for i in range(4)], axis=1)
    rall2 = pieces(rall[...].reshape(4 * tok, rall.shape[2]))

    def partial(core_of):
        want = 16 * ((q // 16) * 8 + x * 2 + core_of) + lax.rem(q, 16)
        hot = jnp.where(want == ids, 1.0, 0.0).astype(BF16)
        return dot_nn(hot, rall2[0]) + dot_nn(hot, rall2[1]) + dot_nn(hot, rall2[2])

    psend[...] = partial(1 - core)
    dcopy = rcopy(psend, precv, ds, dr, partner)
    dcopy.start()
    pown[...] = partial(core)
    lax.fori_loop(n_dev // 4, n_dev // 2, cold, 0)
    dcopy.wait()
    tsend[...] = (pown[...] + precv[...]).reshape(tsend.shape)
    trecv[zy] = tsend[zy]

    def to_yz(d, c):
        other = lax.rem(zy + d, 16)
        rcopy(tsend.at[other], trecv.at[zy], ts, tr, (other * 4 + x) * 2 + core).start()
        return c

    lax.fori_loop(1, 16, to_yz, 0)
    lax.fori_loop(n_dev // 2, n_dev, cold, 0)
    wait_bytes(trecv.at[pl.ds(0, 15)], tr)
    yx = lax.rem(chip, 16)
    dh[z, yx, core] = jnp.sum(trecv[...], axis=0)

    def gather(d, c):
        dev = lax.rem(chip + d, n_dev // 2) * 2 + core
        rcopy(dh.at[z, yx, core], dh.at[z, yx, core], gs, gr.at[z], dev).start()
        return c

    lax.fori_loop(1, n_dev // 2, gather, 0)
    for dz in range(4):
        zz = lax.rem(z + dz, 4)
        n_blk = 15 if dz == 0 else 16
        wait_bytes(dh.at[0, pl.ds(0, n_blk), 0], gr.at[zz])
        rcopy(dh.at[zz, :, core], dh.at[zz, :, core], fs, fr, partner).start()
    ccopy = pltpu.make_async_copy(crecv, cold_ref, osem.at[2])
    wait_bytes(crecv.at[pl.ds(0, n_dev - 1)], cr)
    ccopy.start()
    wait_bytes(dh.at[:, :, 0], fr)
    outs = [pltpu.make_async_copy(dh.at[:, :, :, :, pl.ds(l * 256, 256)], dhot_ref.at[l], osem.at[l]) for l in range(2)]
    for o in outs:
        o.start()
    wait_bytes(rall.at[pl.ds(0, 3)], asem.at[0])
    wait_bytes(iall.at[pl.ds(0, 3)], asem.at[1])
    wait_bytes(csend.at[pl.ds(0, n_dev - 1)], cs)
    wait_bytes(tsend.at[pl.ds(0, 15)], ts)
    wait_bytes(csend.at[pl.ds(0, n_dev - 2)], gs)
    wait_bytes(dh.at[:, :, 0], fs)
    ccopy.wait()
    for o in outs:
        o.wait()


def kt_body(row_ref, cold_ref, out_ref):
    rows = out_ref.shape[1]
    pad = -(-rows // 16) * 16
    it = lax.broadcasted_iota(I32, (pad, row_ref.shape[1]), 0)
    oh = jnp.where(it == row_ref[...], 1.0, 0.0).astype(BF16)
    for l in range(2):
        r = dot3(oh, cold_ref[:, l * 256:(l + 1) * 256])
        out_ref[l] = r[:rows]


def params(cid):
    return pltpu.CompilerParams(collective_id=cid, has_side_effects=True, vmem_limit_bytes=VMEM_LIMIT)


def sds(shape, dt):
    return jax.ShapeDtypeStruct(shape, dt)


DMA = pltpu.SemaphoreType.DMA


def solution(mesh):
    n_dev = mesh.shape['emb']

    def body(token_ids, hot_ids, x_in, d_out, emb_table, hot_table, w_up, w_down, w_gate, w_proj):
        tok, dim = x_in.shape
        _, rows_dev, emb = emb_table.shape
        ff = w_up.shape[2]
        half = ff // 2
        fu, nd = half // N_UP, dim // N_DN
        cap = 8
        n_slots = n_dev * cap
        n_hot = hot_ids.shape[0]
        me = lax.axis_index('emb')
        hot_match = token_ids[:, None] == hot_ids[None, :]
        hidx = jnp.max(jnp.where(hot_match, jnp.arange(n_hot, dtype=I32)[None, :], -1), axis=1)
        is_hot = hidx >= 0
        owner = token_ids // rows_dev
        t = jnp.arange(tok, dtype=I32)
        earlier = (owner[:, None] == owner[None, :]) & ~is_hot[None, :] & (t[None, :] < t[:, None])
        rank = jnp.sum(earlier.astype(I32), axis=1)
        slot = jnp.where(is_hot, -1, owner * cap + rank)
        slot_match = jnp.arange(n_slots, dtype=I32)[:, None] == slot[None, :]
        send_ids = jnp.sum(jnp.where(slot_match, token_ids[None, :] + 1, 0), axis=1) - 1
        recv_ids = lax.all_to_all(send_ids.reshape(n_dev, cap), 'emb', 0, 0, tiled=True).reshape(n_slots)
        local_row = jnp.where(recv_ids >= 0, recv_ids - me * rows_dev, -1)
        row_match = (local_row[:, None] == jnp.arange(rows_dev, dtype=I32)[None, :]).astype(BF16)
        served = jnp.concatenate([dot_nn(row_match, emb_table[l]).astype(BF16) for l in range(2)], axis=1)
        fetched = lax.all_to_all(served.reshape(n_dev, cap, 2 * emb), 'emb', 0, 0, tiled=True).reshape(n_slots, 2 * emb)

        m0, g0 = pl.pallas_call(
            k0_body,
            out_shape=(sds((tok, dim), BF16), sds((tok, emb), BF16)),
            in_specs=[VM, VM, ANY, ANY], out_specs=(VM, VM),
            scratch_shapes=[pltpu.VMEM((tok, dim), BF16), pltpu.VMEM((2 * tok, dim), BF16), pltpu.VMEM((2 * tok, half), BF16),
                            pltpu.VMEM((SLOTS, dim, fu), BF16), pltpu.VMEM((SLOTS, half, nd), BF16),
                            pltpu.VMEM((N_DN, tok, nd), F32), pltpu.VMEM((N_DN, tok, nd), F32), pltpu.VMEM((N_DN, tok, nd), F32),
                            DMA((SLOTS,)), DMA((SLOTS,)), DMA, DMA, DMA((N_DN,)), DMA((N_DN,))],
            compiler_params=params(0), name='dense0',
            cost_estimate=pl.CostEstimate(flops=2 * 2 * 2 * tok * dim * half, bytes_accessed=4 * dim * half, transcendentals=0),
        )(x_in, w_gate[0], w_up, w_down)

        cold = lax.dot_general(slot_match.astype(BF16), fetched, (((0,), (0,)), ((), ())), preferred_element_type=F32)
        hot_oh = hot_match.astype(BF16)
        e = [(cold[:, l * emb:(l + 1) * emb] + dot_nn(hot_oh, hot_table[l])).astype(BF16) for l in range(2)]

        x_out, rows0, rows1 = pl.pallas_call(
            k1_body,
            out_shape=(sds((tok, dim), BF16), sds((tok, emb), F32), sds((tok, emb), F32)),
            in_specs=[VM] * 9 + [ANY] * 2, out_specs=(VM, VM, VM),
            scratch_shapes=[pltpu.VMEM((tok, dim), BF16), pltpu.VMEM((tok, dim), BF16), pltpu.VMEM((2 * tok, dim), BF16),
                            pltpu.VMEM((2 * tok, dim), BF16), pltpu.VMEM((2 * tok, dim), F32), pltpu.VMEM((2 * tok, dim), F32),
                            pltpu.VMEM((tok, dim), F32), pltpu.VMEM((tok, dim), F32),
                            pltpu.VMEM((SLOTS, dim, fu), BF16), pltpu.VMEM((SLOTS, fu, dim), BF16),
                            DMA((SLOTS,)), DMA((SLOTS,)), DMA, DMA, DMA, DMA, DMA, DMA, DMA, DMA],
            compiler_params=params(1), name='dense1',
        )(x_in, m0, g0, e[0], e[1], d_out, w_proj[0], w_gate[1], w_proj[1], w_up, w_down)

        rows = jnp.concatenate([rows0, rows1], axis=1)
        w2 = 2 * emb
        cold_rows, d_hot = pl.pallas_call(
            kh_body,
            out_shape=(sds((n_dev, cap, w2), F32), sds((2, 4, 16, 2, 16, emb), F32)),
            in_specs=[VM] * 3, out_specs=(ANY, ANY),
            scratch_shapes=[pltpu.VMEM((n_dev, cap, w2), F32), pltpu.VMEM((n_dev, cap, w2), F32),
                            pltpu.VMEM((4, tok, w2), F32), pltpu.VMEM((4, 8, tok), I32),
                            pltpu.VMEM((256, w2), F32), pltpu.VMEM((256, w2), F32), pltpu.VMEM((256, w2), F32),
                            pltpu.VMEM((16, 16, w2), F32), pltpu.VMEM((16, 16, w2), F32),
                            pltpu.VMEM((4, 16, 2, 16, w2), F32),
                            DMA((2,)), DMA, DMA, DMA, DMA, DMA, DMA, DMA, DMA, DMA, DMA((4,)), DMA, DMA, DMA((3,))],
            compiler_params=params(2), name='exchange',
        )(rows, hidx.reshape(1, tok), slot.reshape(1, tok))

        d_table = pl.pallas_call(
            kt_body, out_shape=sds((2, rows_dev, emb), F32),
            in_specs=[VM, VM], out_specs=VM,
            compiler_params=pltpu.CompilerParams(vmem_limit_bytes=VMEM_LIMIT), name='table_grad',
        )(local_row.reshape(1, n_slots), cold_rows.reshape(n_slots, w2))
        return x_out, d_table, d_hot.reshape(2, n_hot, emb)

    return jax.shard_map(body, mesh=mesh,
                         in_specs=(P('emb'), P(), P('emb', None), P('emb', None), P(None, 'emb', None), P(), P(), P(), P(), P()),
                         out_specs=(P('emb', None), P(None, 'emb', None), P()),
                         check_vma=False)
```

```python
import functools

import jax
import jax.numpy as jnp
from jax import lax
from jax.experimental import pallas as pl
from jax.experimental.pallas import tpu as pltpu
from jax.sharding import PartitionSpec as P

NORM_EPS = 1e-6
MESH = pl.DeviceIdType.MESH
F32, BF16, I32 = jnp.float32, jnp.bfloat16, jnp.int32
ANY = pl.BlockSpec(memory_space=pl.ANY)
VM = pl.BlockSpec(memory_space=pltpu.VMEM)
GC = 0.7978845608028654
VMEM_LIMIT = 63 * 1024 * 1024


def dot_nn(a, b):
    return jnp.dot(a, b, preferred_element_type=F32)


def dot_nt(a, b):
    return lax.dot_general(a, b, (((1,), (1,)), ((), ())), preferred_element_type=F32)


def gelu(x):
    return 0.5 * x * (1.0 + jnp.tanh(GC * (x + 0.044715 * x * x * x)))


def gelu_both(x):
    x2 = x * x
    t = jnp.tanh(GC * (x + 0.044715 * x * x2))
    half = 0.5 * (1.0 + t)
    return x * half, half + 0.5 * x * (1.0 - t * t) * (GC * (1.0 + 3.0 * 0.044715 * x2))


def rms(xf):
    return lax.rsqrt(jnp.mean(xf * xf, axis=-1, keepdims=True) + NORM_EPS)


def pieces(x):
    hi = x.astype(BF16)
    rest = x - hi.astype(F32)
    mid = rest.astype(BF16)
    return hi, mid, (rest - mid.astype(F32)).astype(BF16)


def dot3(oh, x):
    hi, mid, lo = pieces(x)
    return dot_nn(oh, hi) + dot_nn(oh, mid) + dot_nn(oh, lo)


def rcopy(src, dst, ssem, rsem, dev):
    return pltpu.make_async_remote_copy(src_ref=src, dst_ref=dst, send_sem=ssem, recv_sem=rsem,
                                        device_id=(dev,), device_id_type=MESH)


N_UP = 8
SLOTS = 3
CAP = 8
PIECE = 1024


def wait_bytes(ref, sem):
    pltpu.make_async_copy(ref, ref, sem).wait()


def dot_tn(a, b):
    return lax.dot_general(a, b, (((0,), (0,)), ((), ())), preferred_element_type=F32)


def main_body(rows_dev, x_ref, ids_ref, slot_ref, hidx_ref, emb_ref, hot_ref, wg_ref, wp_ref, d_hbm, wup, wdn,
              xo_ref, rid_ref, cold_ref, dhot_ref,
              up, cp, x1, x1p, act, macc, dacc, mrecv, drecv, wu, wd, ehot, g0s, g1s,
              idr, fsend, frecv, csend, crecv, rall, iall, psend, precv, tsend, trecv, dh,
              wsem, xs, xr, ids_s, ids_r, hs, hr, fs, fr, ash, ar, cs, cr, ps, pr, ts, tr, gs, gr, ks, kr, lsem):
    tok, dim = x_ref.shape
    n_dev = ids_ref.shape[0]
    half = wup.shape[2] // 2
    fu = half // N_UP
    emb = emb_ref.shape[2]
    hb = emb // 2
    me = lax.axis_index('emb')
    core = lax.rem(me, 2)
    chip = me // 2
    x = lax.rem(chip, 4)
    y = lax.rem(chip // 4, 4)
    zy = chip // 4
    z = zy // 4
    partner = me + 1 - 2 * core
    base = core * half
    own, oth = pl.ds(0, tok), pl.ds(tok, tok)

    def w_copies(layer, i, slot):
        off = pl.multiple_of(base + i * fu, fu)
        return (pltpu.make_async_copy(wup.at[layer, :, pl.ds(off, fu)], wu.at[slot], wsem.at[0, slot]),
                pltpu.make_async_copy(wdn.at[layer, pl.ds(off, fu), :], wd.at[slot], wsem.at[1, slot]))

    def w_start(layer, i, slot):
        for c in w_copies(layer, i, slot):
            c.start()

    def to_all(first, last, mk):
        def one(d, c):
            mk(lax.rem(me + d, n_dev)).start()
            return c
        lax.fori_loop(first, last, one, 0)

    for i in range(SLOTS):
        w_start(0, i, i)
    dcopy = pltpu.make_async_copy(d_hbm, cp.at[own], lsem.at[0])
    dcopy.start()
    bar = pltpu.get_barrier_semaphore()

    def sig(d, c):
        pl.semaphore_signal(bar, inc=1, device_id=(lax.rem(me + d, n_dev),), device_id_type=MESH)
        return c

    lax.fori_loop(1, n_dev, sig, 0)
    xf = x_ref[:].astype(F32)
    u = (xf * rms(xf)).astype(BF16)
    up[own, :] = u
    g0s[:] = gelu(dot_nn(u, wg_ref[0]).astype(BF16).astype(F32))
    idr[me] = ids_ref[me]
    iall[x] = jnp.broadcast_to(hidx_ref[:], iall.shape[1:])
    macc[:] = jnp.zeros_like(macc)
    pl.semaphore_wait(bar, n_dev - 1)

    xsend = rcopy(x_ref, x1p, xs.at[0], xr.at[0], partner)
    xsend.start()
    to_all(1, n_dev, lambda dev: rcopy(ids_ref.at[dev], idr.at[me], ids_s, ids_r, dev))
    for d in (1, 3, 2):
        rcopy(iall.at[x], iall.at[x], hs, hr, (zy * 4 + lax.rem(x + d, 4)) * 2 + core).start()
    dcopy.wait()
    csnd = rcopy(cp.at[own], cp.at[oth], xs.at[1], xr.at[1], partner)
    csnd.start()
    hid = lax.broadcasted_iota(I32, (hot_ref.shape[1], tok), 0)
    hoh = jnp.where(hid == hidx_ref[:], 1.0, 0.0).astype(BF16)
    for l in range(2):
        ehot[l] = dot_tn(hoh, hot_ref[l])
    xsend.wait()
    xf = x1p[:].astype(F32)
    up[oth, :] = (xf * rms(xf)).astype(BF16)

    def l0_step(i, c):
        slot = lax.rem(i, SLOTS)
        for cc in w_copies(0, i, slot):
            cc.wait()
        a = gelu(dot_nn(up[:], wu[slot]).astype(BF16).astype(F32)).astype(BF16)
        for n in range(0, dim, PIECE):
            macc[:, n:n + PIECE] += dot_nn(a, wd[slot, :, n:n + PIECE])
        nxt = i + SLOTS

        @pl.when(nxt < N_UP)
        def _():
            w_start(0, nxt, slot)

        @pl.when(nxt >= N_UP)
        def _():
            w_start(1, nxt - N_UP, slot)
        return c

    lax.fori_loop(0, 3, l0_step, 0)

    wait_bytes(idr.at[pl.ds(0, n_dev - 1)], ids_r)
    er = lax.broadcasted_iota(I32, (emb_ref.shape[1], tok), 0)

    def serve(g, c):
        s = jnp.sum(idr[pl.ds(g * 16, 16)], axis=0)
        lr = jnp.where(s > 0, s - 1 - me * rows_dev, -1)
        rid_ref[g] = lr
        oh = jnp.where(er == lr, 1.0, 0.0).astype(BF16)
        for l in range(2):
            sv = dot_tn(oh, emb_ref[l]).reshape(16, CAP, emb)
            fsend[l, pl.ds(g * 16, 16)] = jnp.concatenate([sv[:, :, :hb], sv[:, :, hb:]], axis=1).astype(BF16)
        return c

    lax.fori_loop(0, n_dev // 16, serve, 0)
    for l in range(2):
        frecv[l, me] = fsend[l, me]
        to_all(1, n_dev, lambda dev: rcopy(fsend.at[l, dev], frecv.at[l, me], fs.at[l], fr.at[l], dev))

    lax.fori_loop(3, N_UP, l0_step, 0)
    msend = rcopy(macc.at[oth], mrecv, xs.at[2], xr.at[2], partner)
    msend.start()
    sl = slot_ref[:]
    frow = lax.broadcasted_iota(I32, (n_dev * 16, tok), 0)
    where0 = jnp.where(sl >= 0, (sl // CAP) * 16 + lax.rem(sl, CAP), -16)

    def fetch(l):
        wait_bytes(frecv.at[l, pl.ds(0, n_dev - 1)], fr.at[l])
        f = frecv[l].reshape(n_dev * 16, hb)
        parts = [dot_tn(jnp.where(frow == where0 + h * CAP, 1.0, 0.0).astype(BF16), f) for h in range(2)]
        return (jnp.concatenate(parts, axis=1) + ehot[l]).astype(BF16).astype(F32)

    e0 = fetch(0)
    q = dot_nn((g0s[:].astype(BF16).astype(F32) * e0).astype(BF16), wp_ref[0]).astype(BF16).astype(F32)
    a1 = dot_nt(cp[own, :], wp_ref[1])
    msend.wait()
    m0 = (macc[own, :] + mrecv[:]).astype(BF16).astype(F32)
    x1[:] = (x_ref[:].astype(F32) + m0 + q).astype(BF16)
    csnd.wait()
    xsend1 = rcopy(x1, x1p, xs.at[3], xr.at[3], partner)
    xsend1.start()
    xf = x1[:].astype(F32)
    u = (xf * rms(xf)).astype(BF16)
    up[own, :] = u
    s1 = dot_nn(u, wg_ref[1]).astype(BF16).astype(F32)
    gfull, dgs = gelu_both(s1)
    g1 = gfull.astype(BF16).astype(F32)
    g1s[:] = g1

    def xpeer(d):
        return (zy * 4 + lax.rem(x + d, 4)) * 2 + core

    def cold_copy(l, dev):
        return rcopy(csend.at[dev], crecv.at[l, me], cs.at[l], cr.at[l], dev)

    def rows_out(l, rows):
        rall[l, x] = rows
        for d in (1, 3, 2):
            rcopy(rall.at[l, x], rall.at[l, x], ash.at[l], ar.at[l], xpeer(d)).start()

    def cold_out(l, rows):
        srow = lax.broadcasted_iota(I32, (n_dev * CAP, tok), 0)
        oh = jnp.where(srow == sl, 1.0, 0.0).astype(BF16)
        csend[:] = dot3(oh, rows).reshape(csend.shape)
        crecv[l, me] = csend[me]

    def hot_partial(l):
        wait_bytes(rall.at[l, pl.ds(0, 3)], ar.at[l])
        qi = lax.broadcasted_iota(I32, (256, 4 * tok), 0)
        ids = jnp.concatenate([iall[i, 0:1, :] for i in range(4)], axis=1)
        pc = pieces(rall[l].reshape(4 * tok, emb))

        def partial(core_of):
            want = 16 * ((qi // 16) * 8 + x * 2 + core_of) + lax.rem(qi, 16)
            hot = jnp.where(want == ids, 1.0, 0.0).astype(BF16)
            return dot_nn(hot, pc[0]) + dot_nn(hot, pc[1]) + dot_nn(hot, pc[2])

        psend[l] = partial(1 - core)
        rcopy(psend.at[l], precv.at[l], ps.at[l], pr.at[l], partner).start()
        tsend[l] = partial(core).reshape(tsend.shape[1:])

    def hot_sums(l):
        rcopy(psend.at[l], precv.at[l], ps.at[l], pr.at[l], partner).wait()
        tsend[l] = tsend[l] + precv[l].reshape(tsend.shape[1:])
        trecv[l, zy] = tsend[l, zy]

        def one(d, c):
            other = lax.rem(zy + d, 16)
            rcopy(tsend.at[l, other], trecv.at[l, zy], ts.at[l], tr.at[l], (other * 4 + x) * 2 + core).start()
            return c

        lax.fori_loop(1, 16, one, 0)

    s1c, s2c, s3c = 16 - 15 * core, 4 + 12 * core, 1 + 3 * core
    k1 = z + core * (x - z)
    k2 = y + core * (z - y)
    k3 = x + core * (y - x)

    def blk(a, b, e):
        return a * s1c + b * s2c + e * s3c

    def put(l, src_chip, dst_chip, ssem, rsem):
        ref = dh.at[l, src_chip, core]
        rcopy(ref, ref, ssem, rsem, dst_chip * 2 + core).start()

    def gather1(l):
        wait_bytes(trecv.at[l, pl.ds(0, 15)], tr.at[l])
        dh[l, chip, core] = jnp.sum(trecv[l], axis=0)
        for d in (1, 3, 2):
            put(l, chip, blk(lax.rem(k1 + d, 4), k2, k3), gs.at[l, 0], gr.at[l, 0])

    def gather2(l):
        wait_bytes(dh.at[l, pl.ds(0, 3), 0], gr.at[l, 0])
        for d in (1, 3, 2):
            for a in range(4):
                put(l, blk(a, k2, k3), blk(k1, lax.rem(k2 + d, 4), k3), gs.at[l, 1], gr.at[l, 1])

    def forward(l, e, first=0, last=16):
        def one(i, c):
            ref = dh.at[l, blk(lax.rem(i, 4), i // 4, e), core]
            rcopy(ref, ref, ks.at[l], kr.at[l], partner).start()
            return c
        lax.fori_loop(first, last, one, 0)

    def gather3(l):
        wait_bytes(dh.at[l, pl.ds(0, 12), 0], gr.at[l, 1])
        right, left = lax.rem(k3 + 1, 4), lax.rem(k3 + 3, 4)

        def one(i, c):
            src = blk(lax.rem(i, 4), i // 4, k3)
            put(l, src, blk(k1, k2, right), gs.at[l, 2], gr.at[l, 2])
            put(l, src, blk(k1, k2, left), gs.at[l, 2], gr.at[l, 3])
            return c

        lax.fori_loop(0, 16, one, 0)
        forward(l, k3)

    def gather4(l):
        right, left = lax.rem(k3 + 1, 4), lax.rem(k3 + 3, 4)
        wait_bytes(dh.at[l, pl.ds(0, 16), 0], gr.at[l, 2])

        def pass_right(i, c):
            put(l, blk(lax.rem(i, 4), i // 4, left), blk(k1, k2, right), gs.at[l, 3], gr.at[l, 4])
            return c

        lax.fori_loop(0, 8, pass_right, 0)
        wait_bytes(dh.at[l, pl.ds(0, 16), 0], gr.at[l, 3])

        def pass_left(i, c):
            put(l, blk(lax.rem(i, 4), i // 4, right), blk(k1, k2, left), gs.at[l, 3], gr.at[l, 4])
            return c

        lax.fori_loop(8, 16, pass_left, 0)
        forward(l, left)
        forward(l, right)

    def gather5(l):
        wait_bytes(dh.at[l, pl.ds(0, 16), 0], gr.at[l, 4])
        forward(l, lax.rem(k3 + 2, 4))

    def dhot_out(l):
        wait_bytes(dh.at[l, :, 0], kr.at[l])
        return pltpu.make_async_copy(dh.at[l], dhot_ref.at[l], lsem.at[1 + l])

    def cold_part(l, first, last):
        to_all(max(1, first * 16), last * 16, lambda dev: cold_copy(l, dev))

    rows1 = a1 * g1
    rows_out(1, rows1)
    cold_out(1, rows1)
    cold_part(1, 0, 8)
    macc[:] = jnp.zeros_like(macc)
    dacc[:] = jnp.zeros_like(dacc)
    xsend1.wait()
    xf = x1p[:].astype(F32)
    up[oth, :] = (xf * rms(xf)).astype(BF16)

    def l1_step(i, c):
        slot = lax.rem(i + N_UP, SLOTS)
        for cc in w_copies(1, i, slot):
            cc.wait()
        h = dot_nn(up[:], wu[slot]).astype(BF16).astype(F32)
        a, da = gelu_both(h)
        act[i] = a.astype(BF16)
        dhid = (da * dot_nt(cp[:], wd[slot])).astype(BF16)
        for n in range(0, dim, PIECE):
            dacc[:, n:n + PIECE] += dot_nt(dhid, wu[slot, n:n + PIECE, :])
        nxt = i + SLOTS

        @pl.when(nxt < N_UP)
        def _():
            w_start(1, nxt, slot)

        @pl.when(nxt >= N_UP)
        def _():
            w_copies(1, nxt - N_UP, slot)[1].start()
        return c

    def m_step(i, c):
        slot = lax.rem(i + 2 * N_UP, SLOTS)
        w_copies(1, i, slot)[1].wait()
        for n in range(0, dim, PIECE):
            macc[:, n:n + PIECE] += dot_nn(act[i], wd[slot, :, n:n + PIECE])

        @pl.when(i + SLOTS < N_UP)
        def _():
            w_copies(1, i + SLOTS, slot)[1].start()
        return c

    def m_part(first):
        lax.fori_loop(first, first + 2, m_step, 0)

    lax.fori_loop(0, 6, l1_step, 0)
    wait_bytes(iall.at[pl.ds(0, 3)], hr)
    hot_partial(1)
    e1 = fetch(1)
    du_gate = dot_nt((dgs * (a1 * e1)).astype(BF16), wg_ref[1])
    dacc[own, :] = dacc[own, :] + du_gate
    q1 = dot_nn((g1s[:] * e1).astype(BF16), wp_ref[1]).astype(BF16)
    lax.fori_loop(6, N_UP, l1_step, 0)

    dsend = rcopy(dacc.at[oth], drecv, xs.at[4], xr.at[4], partner)
    dsend.start()
    hot_sums(1)
    xf = x1[:].astype(F32)
    k = rms(xf)
    dsend.wait()
    du = dacc[own, :] + drecv[:]
    inner = jnp.mean(du * xf, axis=-1, keepdims=True)
    r1 = cp[own, :].astype(F32) + k * du - xf * (k * k * k) * inner
    rows0 = dot_nt(r1.astype(BF16), wp_ref[0]) * g0s[:].astype(BF16).astype(F32)
    rows_out(0, rows0)
    wait_bytes(csend.at[pl.ds(0, n_dev - 1)], cs.at[1])
    cold_out(0, rows0)
    cold_part(0, 0, 2)
    gather1(1)
    m_part(0)
    hot_partial(0)
    gather2(1)
    m_part(2)
    hot_sums(0)
    cold_part(0, 2, 4)
    gather3(1)
    wait_bytes(crecv.at[1, pl.ds(0, n_dev - 1)], cr.at[1])
    ccopy1 = pltpu.make_async_copy(crecv.at[1], cold_ref.at[1], lsem.at[3])
    ccopy1.start()
    m_part(4)
    gather1(0)
    cold_part(0, 4, 5)
    gather4(1)
    m_part(6)
    msend = rcopy(macc.at[oth], mrecv, xs.at[5], xr.at[5], partner)
    msend.start()
    gather2(0)
    cold_part(0, 5, 7)
    gather5(1)
    gather3(0)
    cold_part(0, 7, 8)
    out1 = dhot_out(1)
    out1.start()
    msend.wait()
    m1 = (macc[own, :] + mrecv[:]).astype(BF16)
    xo_ref[:] = (xf + m1.astype(F32) + q1.astype(F32)).astype(BF16)
    gather4(0)
    gather5(0)
    wait_bytes(crecv.at[0, pl.ds(0, n_dev - 1)], cr.at[0])
    ccopy0 = pltpu.make_async_copy(crecv.at[0], cold_ref.at[0], lsem.at[4])
    ccopy0.start()
    out0 = dhot_out(0)
    out0.start()
    wait_bytes(idr.at[pl.ds(0, n_dev - 1)], ids_s)
    wait_bytes(iall.at[pl.ds(0, 3)], hs)
    wait_bytes(csend.at[pl.ds(0, n_dev - 1)], cs.at[0])
    for l in range(2):
        wait_bytes(fsend.at[l, pl.ds(0, n_dev - 1)], fs.at[l])
        wait_bytes(rall.at[l, pl.ds(0, 3)], ash.at[l])
        wait_bytes(tsend.at[l, pl.ds(0, 15)], ts.at[l])
        for ph, n_blk in enumerate((3, 12, 32, 16)):
            wait_bytes(dh.at[l, pl.ds(0, n_blk), 0], gs.at[l, ph])
        wait_bytes(dh.at[l, :, 0], ks.at[l])
    for c in (ccopy1, ccopy0, out1, out0):
        c.wait()


def finish_body(rid_ref, cold_ref, x_hbm, dhot_hbm, dt_ref, xo_hbm, dho_hbm, xb, hb, sem):
    rows = dt_ref.shape[0] // 4
    ins = [pltpu.make_async_copy(dhot_hbm.at[l], hb.at[l], sem.at[l]) for l in range(2)]
    ins.append(pltpu.make_async_copy(x_hbm, xb, sem.at[2]))
    for c in ins:
        c.start()
    ids = jnp.concatenate([rid_ref[g] for g in range(rid_ref.shape[0])], axis=1)
    outs = [pltpu.make_async_copy(hb.at[l], dho_hbm.at[l], sem.at[3 + l]) for l in range(2)]
    outs.append(pltpu.make_async_copy(xb, xo_hbm, sem.at[5]))
    step = 336
    for l in range(2):
        pc = pieces(cold_ref[l])
        for r0 in range(0, rows, step):
            it = lax.broadcasted_iota(I32, (step, ids.shape[1]), 0) + r0
            oh = jnp.where(it == ids, 1.0, 0.0).astype(BF16)
            r = dot_nn(oh, pc[0]) + dot_nn(oh, pc[1]) + dot_nn(oh, pc[2])
            n = min(step, rows - r0)
            for t in range(2):
                dt_ref[pl.ds(r0 * 4 + t * 2 + l, n, stride=4), :] = r[:n, t * 128:(t + 1) * 128]
        if l == 0:
            for i, o in zip(ins, outs):
                i.wait()
                o.start()
    for o in outs:
        o.wait()


def sds(shape, dt):
    return jax.ShapeDtypeStruct(shape, dt)


DMA = pltpu.SemaphoreType.DMA


def solution(mesh):
    n_dev = mesh.shape['emb']

    def body(token_ids, hot_ids, x_in, d_out, emb_table, hot_table, w_up, w_down, w_gate, w_proj):
        tok, dim = x_in.shape
        _, rows_dev, emb = emb_table.shape
        half = w_up.shape[2] // 2
        fu = half // N_UP
        n_hot = hot_ids.shape[0]
        n_slots = n_dev * CAP
        me = lax.axis_index('emb')
        hot_match = token_ids[:, None] == hot_ids[None, :]
        hidx = jnp.max(jnp.where(hot_match, jnp.arange(n_hot, dtype=I32)[None, :], -1), axis=1)
        is_hot = hidx >= 0
        owner = token_ids // rows_dev
        t = jnp.arange(tok, dtype=I32)
        earlier = (owner[:, None] == owner[None, :]) & ~is_hot[None, :] & (t[None, :] < t[:, None])
        rank = jnp.sum(earlier.astype(I32), axis=1)
        slot = jnp.where(is_hot, -1, owner * CAP + rank)
        lane = lax.rem(me, 16) * CAP + rank
        o_hit = (jnp.arange(n_dev, dtype=I32)[:, None] == jnp.where(is_hot, -1, owner)[None, :]).astype(BF16)
        l_hit = t[None, :] == lane[:, None]
        want_id = token_ids + 1
        hi, lo = want_id // 512, want_id % 512
        put = [jnp.where(l_hit, v[:, None], 0).astype(BF16) for v in (hi, lo // 2, lo % 2)]
        got = [dot_nn(o_hit, v).astype(I32) for v in put]
        send_ids = got[0] * 512 + got[1] * 2 + got[2]
        emb_pad = jnp.pad(emb_table, ((0, 0), (0, -rows_dev % 16), (0, 0)))

        VMEM = pltpu.VMEM
        x_raw, rid, cold, dhot = pl.pallas_call(
            functools.partial(main_body, rows_dev),
            out_shape=(sds((tok, dim), BF16), sds((n_dev // 16, 1, 128), I32), sds((2, n_dev, CAP, emb), F32),
                       sds((2, n_dev // 2, 2, 16, emb), F32)),
            in_specs=[VM] * 8 + [ANY] * 3, out_specs=(VM, VM, ANY, ANY),
            scratch_shapes=[VMEM((2 * tok, dim), BF16), VMEM((2 * tok, dim), BF16), VMEM((tok, dim), BF16), VMEM((tok, dim), BF16), VMEM((N_UP, 2 * tok, fu), BF16),
                            VMEM((2 * tok, dim), F32), VMEM((2 * tok, dim), F32), VMEM((tok, dim), F32), VMEM((tok, dim), F32),
                            VMEM((SLOTS, dim, fu), BF16), VMEM((SLOTS, fu, dim), BF16),
                            VMEM((2, tok, emb), F32), VMEM((tok, emb), F32), VMEM((tok, emb), F32),
                            VMEM((n_dev, 1, 128), I32), VMEM((2, n_dev, 16, 128), BF16), VMEM((2, n_dev, 16, 128), BF16),
                            VMEM((n_dev, CAP, emb), F32), VMEM((2, n_dev, CAP, emb), F32),
                            VMEM((2, 4, tok, emb), F32), VMEM((4, 8, tok), I32),
                            VMEM((2, 256, emb), F32), VMEM((2, 256, emb), F32),
                            VMEM((2, 16, 16, emb), F32), VMEM((2, 16, 16, emb), F32),
                            VMEM((2, n_dev // 2, 2, 16, emb), F32),
                            DMA((2, SLOTS)), DMA((6,)), DMA((6,)), DMA, DMA, DMA, DMA] + [DMA((2,))] * 10
            + [DMA((2, 4)), DMA((2, 5)), DMA((2,)), DMA((2,)), DMA((5,))],
            compiler_params=pltpu.CompilerParams(collective_id=0, has_side_effects=True, vmem_limit_bytes=VMEM_LIMIT),
            name='stack',
        )(x_in, send_ids.reshape(n_dev, 1, 128), slot.reshape(1, tok), hidx.reshape(1, tok), emb_pad, hot_table, w_gate, w_proj,
          d_out, w_up, w_down)

        d_table, x_out, d_hot = pl.pallas_call(
            finish_body,
            out_shape=(sds((rows_dev * 4, 128), F32), sds((tok, dim), BF16), sds((2, n_hot, emb), F32)),
            in_specs=[VM, VM, ANY, ANY], out_specs=(VM, ANY, ANY),
            scratch_shapes=[VMEM((tok, dim), BF16), VMEM((2, n_hot, emb), F32), DMA((6,))],
            compiler_params=pltpu.CompilerParams(vmem_limit_bytes=VMEM_LIMIT), name='finish',
        )(rid, cold.reshape(2, n_slots, emb), x_raw, dhot.reshape(2, n_hot, emb))
        d_table = d_table.reshape(rows_dev, 2, 2, 128).transpose(2, 0, 1, 3).reshape(2, rows_dev, emb)
        return x_out, d_table, d_hot

    return jax.shard_map(body, mesh=mesh,
                         in_specs=(P('emb'), P(), P('emb', None), P('emb', None), P(None, 'emb', None), P(), P(), P(), P(), P()),
                         out_specs=(P('emb', None), P(None, 'emb', None), P()),
                         check_vma=False)
```

```python
import functools

import jax
import jax.numpy as jnp
from jax import lax
from jax.experimental import pallas as pl
from jax.experimental.pallas import tpu as pltpu
from jax.sharding import PartitionSpec as P

NORM_EPS = 1e-6
MESH = pl.DeviceIdType.MESH
F32, BF16, I32 = jnp.float32, jnp.bfloat16, jnp.int32
ANY = pl.BlockSpec(memory_space=pl.ANY)
VM = pl.BlockSpec(memory_space=pltpu.VMEM)
GC = 0.7978845608028654
VMEM_LIMIT = 67043328


def dot_nn(a, b):
    return jnp.dot(a, b, preferred_element_type=F32)


def dot_nt(a, b):
    return lax.dot_general(a, b, (((1,), (1,)), ((), ())), preferred_element_type=F32)


def gelu(x):
    return 0.5 * x * (1.0 + jnp.tanh(GC * (x + 0.044715 * x * x * x)))


def gelu_both(x):
    x2 = x * x
    t = jnp.tanh(GC * (x + 0.044715 * x * x2))
    half = 0.5 * (1.0 + t)
    return x * half, half + 0.5 * x * (1.0 - t * t) * (GC * (1.0 + 3.0 * 0.044715 * x2))


def rms(xf):
    return lax.rsqrt(jnp.mean(xf * xf, axis=-1, keepdims=True) + NORM_EPS)


def head(n):
    return pl.ds(0, n)


def one_hot(mask):
    return jnp.where(mask, 1.0, 0.0).astype(BF16)


def pieces(x):
    hi = x.astype(BF16)
    rest = x - hi.astype(F32)
    mid = rest.astype(BF16)
    return hi, mid, (rest - mid.astype(F32)).astype(BF16)


def dot3(oh, x):
    hi, mid, lo = pieces(x)
    return dot_nn(oh, hi) + dot_nn(oh, mid) + dot_nn(oh, lo)


def rcopy(src, dst, ssem, rsem, dev):
    return pltpu.make_async_remote_copy(src_ref=src, dst_ref=dst, send_sem=ssem, recv_sem=rsem,
                                        device_id=(dev,), device_id_type=MESH)


N_UP = 8
SLOTS = 3
CAP = 8
PIECE = 1024


def wait_bytes(ref, sem):
    pltpu.make_async_copy(ref, ref, sem).wait()


def dot_tn(a, b):
    return lax.dot_general(a, b, (((0,), (0,)), ((), ())), preferred_element_type=F32)


def main_body(rows_dev, x_ref, ids_ref, slot_ref, hidx_ref, emb_ref, hot_ref, wg_ref, wp_ref, d_hbm, wup, wdn,
              xo_ref, dt_ref, dhot_ref,
              up, cp, x1, x1p, act, macc, dacc, mrecv, drecv, wu, wd, ehot, g0s, g1s,
              rid, idr, fsend, frecv, csend, crecv, rall, iall, psend, precv, tsend, trecv, dh,
              wsem, xs, xr, ids_s, ids_r, hs, hr, fs, fr, ash, arl, ar, cs, cr, ps, pr, ts, tr, gs, gr, ks, kr, lsem):
    tok, dim = x_ref.shape
    n_dev = ids_ref.shape[0]
    half = wup.shape[2] // 2
    fu = half // N_UP
    emb = emb_ref.shape[2]
    hb = emb // 2
    me = lax.axis_index('emb')
    core = lax.rem(me, 2)
    chip = me // 2
    x = lax.rem(chip, 4)
    y = lax.rem(chip // 4, 4)
    zy = chip // 4
    z = zy // 4
    partner = me + 1 - 2 * core
    base = core * half
    own, oth = head(tok), pl.ds(tok, tok)

    def w_copies(layer, i, slot):
        off = pl.multiple_of(base + i * fu, fu)
        return (pltpu.make_async_copy(wup.at[layer, :, pl.ds(off, fu)], wu.at[slot], wsem.at[0, slot]),
                pltpu.make_async_copy(wdn.at[layer, pl.ds(off, fu), :], wd.at[slot], wsem.at[1, slot]))

    def w_start(layer, i, slot):
        for c in w_copies(layer, i, slot):
            c.start()

    def to_all(first, last, mk):
        def one(d, c):
            mk(lax.rem(me + d, n_dev)).start()
            return c
        lax.fori_loop(first, last, one, 0)

    for i in range(SLOTS):
        w_start(0, i, i)
    dcopy = pltpu.make_async_copy(d_hbm, cp.at[own], lsem.at[0])
    dcopy.start()
    bar = pltpu.get_barrier_semaphore()

    def sig(d, c):
        pl.semaphore_signal(bar, inc=1, device_id=(lax.rem(me + d, n_dev),), device_id_type=MESH)
        return c

    lax.fori_loop(1, n_dev, sig, 0)
    xf = x_ref[:].astype(F32)
    u = (xf * rms(xf)).astype(BF16)
    up[own, :] = u
    g0s[:] = gelu(dot_nn(u, wg_ref[0]).astype(BF16).astype(F32))
    idr[me] = ids_ref[me]
    iall[x] = jnp.broadcast_to(hidx_ref[:], iall.shape[1:])
    macc[:] = jnp.zeros_like(macc)
    pl.semaphore_wait(bar, n_dev - 1)

    xsend = rcopy(x_ref, x1p, xs.at[0], xr.at[0], partner)
    xsend.start()
    to_all(1, n_dev, lambda dev: rcopy(ids_ref.at[dev], idr.at[me], ids_s, ids_r, dev))
    for d in (1, 3, 2):
        rcopy(iall.at[x], iall.at[x], hs, hr, (zy * 4 + lax.rem(x + d, 4)) * 2 + core).start()
    dcopy.wait()
    csnd = rcopy(cp.at[own], cp.at[oth], xs.at[1], xr.at[1], partner)
    csnd.start()
    hid = lax.broadcasted_iota(I32, (hot_ref.shape[1], tok), 0)
    hoh = one_hot(hid == hidx_ref[:])
    for l in range(2):
        ehot[l] = dot_tn(hoh, hot_ref[l])
    xsend.wait()
    xf = x1p[:].astype(F32)
    up[oth, :] = (xf * rms(xf)).astype(BF16)

    def l0_step(i, c):
        slot = lax.rem(i, SLOTS)
        for cc in w_copies(0, i, slot):
            cc.wait()
        a = gelu(dot_nn(up[:], wu[slot]).astype(BF16).astype(F32)).astype(BF16)
        for n in range(0, dim, PIECE):
            macc[:, n:n + PIECE] += dot_nn(a, wd[slot, :, n:n + PIECE])
        nxt = i + SLOTS

        @pl.when(nxt < N_UP)
        def _():
            w_start(0, nxt, slot)

        @pl.when(nxt >= N_UP)
        def _():
            w_start(1, nxt - N_UP, slot)
        return c

    lax.fori_loop(0, 3, l0_step, 0)

    wait_bytes(idr.at[head(n_dev - 1)], ids_r)
    er = lax.broadcasted_iota(I32, (emb_ref.shape[1], tok), 0)

    def serve(g, c):
        s = jnp.sum(idr[pl.ds(g * 16, 16)], axis=0)
        lr = jnp.where(s > 0, s - 1 - me * rows_dev, -1)
        rid[g] = lr
        oh = one_hot(er == lr)
        for l in range(2):
            sv = dot_tn(oh, emb_ref[l]).reshape(16, CAP, emb)
            fsend[l, pl.ds(g * 16, 16)] = jnp.concatenate([sv[:, :, :hb], sv[:, :, hb:]], axis=1).astype(BF16)
        return c

    lax.fori_loop(0, n_dev // 16, serve, 0)
    for l in range(2):
        frecv[l, me] = fsend[l, me]
        to_all(1, n_dev, lambda dev: rcopy(fsend.at[l, dev], frecv.at[l, me], fs.at[l], fr.at[l], dev))

    lax.fori_loop(3, N_UP, l0_step, 0)
    msend = rcopy(macc.at[oth], mrecv, xs.at[2], xr.at[2], partner)
    msend.start()
    sl = slot_ref[:]
    frow = lax.broadcasted_iota(I32, (n_dev * 16, tok), 0)
    where0 = jnp.where(sl >= 0, (sl // CAP) * 16 + lax.rem(sl, CAP), -16)

    def fetch(l):
        wait_bytes(frecv.at[l, head(n_dev - 1)], fr.at[l])
        f = frecv[l].reshape(n_dev * 16, hb)
        parts = [dot_tn(one_hot(frow == where0 + h * CAP), f) for h in range(2)]
        return (jnp.concatenate(parts, axis=1) + ehot[l]).astype(BF16).astype(F32)

    e0 = fetch(0)
    q = dot_nn((g0s[:].astype(BF16).astype(F32) * e0).astype(BF16), wp_ref[0]).astype(BF16).astype(F32)
    a1 = dot_nt(cp[own, :], wp_ref[1])
    msend.wait()
    m0 = (macc[own, :] + mrecv[:]).astype(BF16).astype(F32)
    x1[:] = (x_ref[:].astype(F32) + m0 + q).astype(BF16)
    csnd.wait()
    xsend1 = rcopy(x1, x1p, xs.at[3], xr.at[3], partner)
    xsend1.start()
    xf = x1[:].astype(F32)
    u = (xf * rms(xf)).astype(BF16)
    up[own, :] = u
    s1 = dot_nn(u, wg_ref[1]).astype(BF16).astype(F32)
    gfull, dgs = gelu_both(s1)
    g1 = gfull.astype(BF16).astype(F32)
    g1s[:] = g1

    def xpeer(d):
        return (zy * 4 + lax.rem(x + d, 4)) * 2 + core

    def cold_copy(l, dev):
        return rcopy(csend.at[dev], crecv.at[l, me], cs.at[l], cr.at[l], dev)

    def rows_out(l, rows):
        rall[l, x] = rows
        rcopy(rall.at[l, x], rall.at[l, x], ash.at[l], ar.at[l, 0], xpeer(1)).start()
        rcopy(rall.at[l, x], rall.at[l, x], ash.at[l], ar.at[l, 1], xpeer(3)).start()

    def rows_relay(l):
        mid = tok // 2
        wait_bytes(rall.at[l, 0], ar.at[l, 0])
        ref = rall.at[l, lax.rem(x + 3, 4), head(mid)]
        rcopy(ref, ref, arl.at[l], ar.at[l, 2], xpeer(1)).start()
        wait_bytes(rall.at[l, 0], ar.at[l, 1])
        ref = rall.at[l, lax.rem(x + 1, 4), pl.ds(mid, mid)]
        rcopy(ref, ref, arl.at[l], ar.at[l, 2], xpeer(3)).start()

    def cold_out(l, rows):
        srow = lax.broadcasted_iota(I32, (n_dev * CAP, tok), 0)
        oh = one_hot(srow == sl)
        csend[:] = dot3(oh, rows).reshape(csend.shape)
        crecv[l, me] = csend[me]

    def hot_partial(l):
        wait_bytes(rall.at[l, 0], ar.at[l, 2])
        qi = lax.broadcasted_iota(I32, (256, 4 * tok), 0)
        ids = jnp.concatenate([iall[i, 0:1, :] for i in range(4)], axis=1)
        pc = pieces(rall[l].reshape(4 * tok, emb))

        def partial(core_of):
            want = 16 * ((qi // 16) * 8 + x * 2 + core_of) + lax.rem(qi, 16)
            hot = one_hot(want == ids)
            return dot_nn(hot, pc[0]) + dot_nn(hot, pc[1]) + dot_nn(hot, pc[2])

        psend[l] = partial(1 - core)
        rcopy(psend.at[l], precv.at[l], ps.at[l], pr.at[l], partner).start()
        tsend[l] = partial(core).reshape(tsend.shape[1:])

    def hot_sums(l):
        rcopy(psend.at[l], precv.at[l], ps.at[l], pr.at[l], partner).wait()
        tsend[l] = tsend[l] + precv[l].reshape(tsend.shape[1:])
        trecv[l, zy] = tsend[l, zy]

        def one(d, c):
            other = lax.rem(zy + d, 16)
            rcopy(tsend.at[l, other], trecv.at[l, zy], ts.at[l], tr.at[l], (other * 4 + x) * 2 + core).start()
            return c

        lax.fori_loop(1, 16, one, 0)

    s1c, s2c, s3c = 16 - 15 * core, 4 + 12 * core, 1 + 3 * core
    k1 = z + core * (x - z)
    k2 = y + core * (z - y)
    k3 = x + core * (y - x)

    def blk(a, b, e):
        return a * s1c + b * s2c + e * s3c

    def put(l, src_chip, dst_chip, ssem, rsem):
        ref = dh.at[l, src_chip, core]
        rcopy(ref, ref, ssem, rsem, dst_chip * 2 + core).start()

    def gather1(l):
        wait_bytes(trecv.at[l, head(15)], tr.at[l])
        dh[l, chip, core] = jnp.sum(trecv[l], axis=0)
        for d in (1, 3, 2):
            put(l, chip, blk(lax.rem(k1 + d, 4), k2, k3), gs.at[l, 0], gr.at[l, 0])

    def gather2(l):
        wait_bytes(dh.at[l, head(3), 0], gr.at[l, 0])
        for d in (1, 3, 2):
            for a in range(4):
                put(l, blk(a, k2, k3), blk(k1, lax.rem(k2 + d, 4), k3), gs.at[l, 1], gr.at[l, 1])

    def forward(l, e, first=0, last=16):
        def one(i, c):
            ref = dh.at[l, blk(lax.rem(i, 4), i // 4, e), core]
            rcopy(ref, ref, ks.at[l], kr.at[l], partner).start()
            return c
        lax.fori_loop(first, last, one, 0)

    def gather3(l):
        wait_bytes(dh.at[l, head(12), 0], gr.at[l, 1])
        right, left = lax.rem(k3 + 1, 4), lax.rem(k3 + 3, 4)

        def one(i, c):
            src = blk(lax.rem(i, 4), i // 4, k3)
            put(l, src, blk(k1, k2, right), gs.at[l, 2], gr.at[l, 2])
            put(l, src, blk(k1, k2, left), gs.at[l, 2], gr.at[l, 3])
            return c

        lax.fori_loop(0, 16, one, 0)
        forward(l, k3)

    def gather4(l):
        right, left = lax.rem(k3 + 1, 4), lax.rem(k3 + 3, 4)
        wait_bytes(dh.at[l, head(16), 0], gr.at[l, 2])

        def pass_right(i, c):
            put(l, blk(lax.rem(i, 4), i // 4, left), blk(k1, k2, right), gs.at[l, 3], gr.at[l, 4])
            return c

        lax.fori_loop(0, 8, pass_right, 0)
        wait_bytes(dh.at[l, head(16), 0], gr.at[l, 3])

        def pass_left(i, c):
            put(l, blk(lax.rem(i, 4), i // 4, right), blk(k1, k2, left), gs.at[l, 3], gr.at[l, 4])
            return c

        lax.fori_loop(8, 16, pass_left, 0)
        forward(l, left)
        forward(l, right)

    def gather5(l):
        wait_bytes(dh.at[l, head(16), 0], gr.at[l, 4])
        forward(l, lax.rem(k3 + 2, 4))

    def dhot_out(l):
        wait_bytes(dh.at[l, :, 0], kr.at[l])
        return pltpu.make_async_copy(dh.at[l], dhot_ref.at[l], lsem.at[1 + l])

    def table(l):
        wait_bytes(crecv.at[l, head(n_dev - 1)], cr.at[l])
        ids = jnp.concatenate([rid[g] for g in range(n_dev // 16)], axis=1)
        pc = pieces(crecv[l].reshape(n_dev * CAP, emb))
        wide = 4 * emb
        for j in range(4):
            ri = lax.broadcasted_iota(I32, (2 * tok, n_dev * CAP), 0) + j * 2 * tok
            oh = one_hot(ri == ids)
            c0 = l * wide + j * emb
            dacc[:, c0:c0 + emb] = dot_nn(oh, pc[0]) + dot_nn(oh, pc[1]) + dot_nn(oh, pc[2])
        cols = pl.ds(l * wide, wide)
        return pltpu.make_async_copy(dacc.at[:, cols], dt_ref.at[:, cols], lsem.at[3 + l])

    def cold_part(l, first, last):
        to_all(max(1, first * 16), last * 16, lambda dev: cold_copy(l, dev))

    rows1 = a1 * g1
    rows_out(1, rows1)
    cold_out(1, rows1)
    cold_part(1, 0, 8)
    macc[:] = jnp.zeros_like(macc)
    dacc[:] = jnp.zeros_like(dacc)
    xsend1.wait()
    xf = x1p[:].astype(F32)
    up[oth, :] = (xf * rms(xf)).astype(BF16)

    def l1_step(i, c):
        slot = lax.rem(i + N_UP, SLOTS)
        for cc in w_copies(1, i, slot):
            cc.wait()
        h = dot_nn(up[:], wu[slot]).astype(BF16).astype(F32)
        a, da = gelu_both(h)
        act[i] = a.astype(BF16)
        dhid = (da * dot_nt(cp[:], wd[slot])).astype(BF16)
        for n in range(0, dim, PIECE):
            dacc[:, n:n + PIECE] += dot_nt(dhid, wu[slot, n:n + PIECE, :])
        nxt = i + SLOTS

        @pl.when(nxt < N_UP)
        def _():
            w_start(1, nxt, slot)

        @pl.when(nxt >= N_UP)
        def _():
            w_copies(1, nxt - N_UP, slot)[1].start()
        return c

    def m_step(i, c):
        slot = lax.rem(i + 2 * N_UP, SLOTS)
        w_copies(1, i, slot)[1].wait()
        for n in range(0, dim, PIECE):
            macc[:, n:n + PIECE] += dot_nn(act[i], wd[slot, :, n:n + PIECE])

        @pl.when(i + SLOTS < N_UP)
        def _():
            w_copies(1, i + SLOTS, slot)[1].start()
        return c

    def m_part(first):
        lax.fori_loop(first, first + 2, m_step, 0)

    lax.fori_loop(0, 3, l1_step, 0)
    rows_relay(1)
    lax.fori_loop(3, 6, l1_step, 0)
    wait_bytes(iall.at[head(3)], hr)
    hot_partial(1)
    e1 = fetch(1)
    du_gate = dot_nt((dgs * (a1 * e1)).astype(BF16), wg_ref[1])
    dacc[own, :] = dacc[own, :] + du_gate
    q1 = dot_nn((g1s[:] * e1).astype(BF16), wp_ref[1]).astype(BF16)
    lax.fori_loop(6, N_UP, l1_step, 0)

    dsend = rcopy(dacc.at[oth], drecv, xs.at[4], xr.at[4], partner)
    dsend.start()
    hot_sums(1)
    xf = x1[:].astype(F32)
    k = rms(xf)
    dsend.wait()
    du = dacc[own, :] + drecv[:]
    inner = jnp.mean(du * xf, axis=-1, keepdims=True)
    r1 = cp[own, :].astype(F32) + k * du - xf * (k * k * k) * inner
    rows0 = dot_nt(r1.astype(BF16), wp_ref[0]) * g0s[:].astype(BF16).astype(F32)
    rows_out(0, rows0)
    wait_bytes(csend.at[head(n_dev - 1)], cs.at[1])
    cold_out(0, rows0)
    cold_part(0, 0, 2)
    gather1(1)
    m_part(0)
    rows_relay(0)
    gather2(1)
    m_part(2)
    hot_partial(0)
    m_part(4)
    hot_sums(0)
    cold_part(0, 2, 5)
    gather3(1)
    m_part(6)
    msend = rcopy(macc.at[oth], mrecv, xs.at[5], xr.at[5], partner)
    msend.start()
    gather1(0)
    cold_part(0, 5, 7)
    gather4(1)
    gather2(0)
    cold_part(0, 7, 8)
    ccopy1 = table(1)
    ccopy1.start()
    gather5(1)
    gather3(0)
    out1 = dhot_out(1)
    out1.start()
    msend.wait()
    m1 = (macc[own, :] + mrecv[:]).astype(BF16)
    xo_ref[:] = (xf + m1.astype(F32) + q1.astype(F32)).astype(BF16)
    gather4(0)
    ccopy0 = table(0)
    ccopy0.start()
    gather5(0)
    out0 = dhot_out(0)
    out0.start()
    wait_bytes(idr.at[head(n_dev - 1)], ids_s)
    wait_bytes(iall.at[head(3)], hs)
    wait_bytes(csend.at[head(n_dev - 1)], cs.at[0])
    for l in range(2):
        wait_bytes(fsend.at[l, head(n_dev - 1)], fs.at[l])
        wait_bytes(rall.at[l, head(2)], ash.at[l])
        wait_bytes(rall.at[l, 0], arl.at[l])
        wait_bytes(tsend.at[l, head(15)], ts.at[l])
        for ph, n_blk in enumerate((3, 12, 32, 16)):
            wait_bytes(dh.at[l, head(n_blk), 0], gs.at[l, ph])
        wait_bytes(dh.at[l, :, 0], ks.at[l])
    for c in (ccopy1, ccopy0, out1, out0):
        c.wait()


def finish_body(raw_ref, x_hbm, dhot_hbm, dt_ref, xo_hbm, dho_hbm, xb, hb, sem):
    rows = dt_ref.shape[0] // 4
    step, wide = raw_ref.shape[0], raw_ref.shape[1] // 2
    moves = [(dhot_hbm.at[l], hb.at[l], dho_hbm.at[l]) for l in range(2)] + [(x_hbm, xb, xo_hbm)]
    ins = [pltpu.make_async_copy(src, buf, sem.at[0, i]) for i, (src, buf, _) in enumerate(moves)]
    outs = [pltpu.make_async_copy(buf, dst, sem.at[1, i]) for i, (_, buf, dst) in enumerate(moves)]
    for c in ins:
        c.start()
    for l in range(2):
        for j in range(4):
            n = min(step, rows - j * step)
            for t in range(2):
                c0 = l * wide + j * 256 + t * 128
                dt_ref[pl.ds(j * step * 4 + t * 2 + l, n, stride=4), :] = raw_ref[0:n, c0:c0 + 128]
        if l == 0:
            for i, o in zip(ins, outs):
                i.wait()
                o.start()
    for o in outs:
        o.wait()


def sds(shape, dt):
    return jax.ShapeDtypeStruct(shape, dt)


DMA = pltpu.SemaphoreType.DMA


def solution(mesh):
    n_dev = mesh.shape['emb']

    def body(token_ids, hot_ids, x_in, d_out, emb_table, hot_table, w_up, w_down, w_gate, w_proj):
        tok, dim = x_in.shape
        _, rows_dev, emb = emb_table.shape
        half = w_up.shape[2] // 2
        fu = half // N_UP
        n_hot = hot_ids.shape[0]
        me = lax.axis_index('emb')
        hot_match = token_ids[:, None] == hot_ids[None, :]
        hidx = jnp.max(jnp.where(hot_match, jnp.arange(n_hot, dtype=I32)[None, :], -1), axis=1)
        is_hot = hidx >= 0
        owner = token_ids // rows_dev
        t = jnp.arange(tok, dtype=I32)
        earlier = (owner[:, None] == owner[None, :]) & ~is_hot[None, :] & (t[None, :] < t[:, None])
        rank = jnp.sum(earlier.astype(I32), axis=1)
        slot = jnp.where(is_hot, -1, owner * CAP + rank)
        lane = lax.rem(me, 16) * CAP + rank
        o_hit = (jnp.arange(n_dev, dtype=I32)[:, None] == jnp.where(is_hot, -1, owner)[None, :]).astype(BF16)
        l_hit = t[None, :] == lane[:, None]
        want_id = token_ids + 1
        hi, lo = want_id // 512, want_id % 512
        put = [jnp.where(l_hit, v[:, None], 0).astype(BF16) for v in (hi, lo // 2, lo % 2)]
        got = [dot_nn(o_hit, v).astype(I32) for v in put]
        send_ids = got[0] * 512 + got[1] * 2 + got[2]
        emb_pad = jnp.pad(emb_table, ((0, 0), (0, -rows_dev % 16), (0, 0)))

        VMEM = pltpu.VMEM
        x_raw, dt_raw, dhot = pl.pallas_call(
            functools.partial(main_body, rows_dev),
            out_shape=(sds((tok, dim), BF16), sds((2 * tok, 8 * emb), F32),
                       sds((2, n_dev // 2, 2, 16, emb), F32)),
            in_specs=[VM] * 8 + [ANY] * 3, out_specs=(VM, ANY, ANY),
            scratch_shapes=[VMEM((2 * tok, dim), BF16), VMEM((2 * tok, dim), BF16), VMEM((tok, dim), BF16), VMEM((tok, dim), BF16), VMEM((N_UP, 2 * tok, fu), BF16),
                            VMEM((2 * tok, dim), F32), VMEM((2 * tok, dim), F32), VMEM((tok, dim), F32), VMEM((tok, dim), F32),
                            VMEM((SLOTS, dim, fu), BF16), VMEM((SLOTS, fu, dim), BF16),
                            VMEM((2, tok, emb), F32), VMEM((tok, emb), F32), VMEM((tok, emb), F32),
                            VMEM((n_dev // 16, 1, 128), I32), VMEM((n_dev, 1, 128), I32), VMEM((2, n_dev, 16, 128), BF16), VMEM((2, n_dev, 16, 128), BF16),
                            VMEM((n_dev, CAP, emb), F32), VMEM((2, n_dev, CAP, emb), F32),
                            VMEM((2, 4, tok, emb), F32), VMEM((4, 8, tok), I32),
                            VMEM((2, 256, emb), F32), VMEM((2, 256, emb), F32),
                            VMEM((2, 16, 16, emb), F32), VMEM((2, 16, 16, emb), F32),
                            VMEM((2, n_dev // 2, 2, 16, emb), F32),
                            DMA((2, SLOTS)), DMA((6,)), DMA((6,)), DMA, DMA, DMA, DMA] + [DMA((2,))] * 4 + [DMA((2, 3))] + [DMA((2,))] * 6
            + [DMA((2, 4)), DMA((2, 5)), DMA((2,)), DMA((2,)), DMA((5,))],
            compiler_params=pltpu.CompilerParams(collective_id=0, has_side_effects=True, vmem_limit_bytes=VMEM_LIMIT),
            name='stack',
        )(x_in, send_ids.reshape(n_dev, 1, 128), slot.reshape(1, tok), hidx.reshape(1, tok), emb_pad, hot_table, w_gate, w_proj,
          d_out, w_up, w_down)

        d_table, x_out, d_hot = pl.pallas_call(
            finish_body,
            out_shape=(sds((rows_dev * 4, 128), F32), sds((tok, dim), BF16), sds((2, n_hot, emb), F32)),
            in_specs=[VM, ANY, ANY], out_specs=(VM, ANY, ANY),
            scratch_shapes=[VMEM((tok, dim), BF16), VMEM((2, n_hot, emb), F32), DMA((2, 3))],
            compiler_params=pltpu.CompilerParams(vmem_limit_bytes=VMEM_LIMIT), name='finish',
        )(dt_raw, x_raw, dhot.reshape(2, n_hot, emb))
        d_table = d_table.reshape(rows_dev, 2, 2, 128).transpose(2, 0, 1, 3).reshape(2, rows_dev, emb)
        return x_out, d_table, d_hot

    return jax.shard_map(body, mesh=mesh,
                         in_specs=(P('emb'), P(), P('emb', None), P('emb', None), P(None, 'emb', None), P(), P(), P(), P(), P()),
                         out_specs=(P('emb', None), P(None, 'emb', None), P()),
                         check_vma=False)
```
